32 devices in a mesh: dp: 2 (over x), vocab: 16 (over z, y, core).
Axes of the slice: x: 2, y: 2, z: 4, core: 2. Of those that a mesh axis runs over, the one named last changes fastest.
Arguments:
- hidden: bfloat16 [1536, 4096], P(('dp', 'vocab')), may hold values from -75 to 75
- embedding: bfloat16 [8192, 4096], P(('dp', 'vocab')), may hold values from -0.5 to 0.5
- targets: int32 [1536], replicated, may hold values from 0 to 8191
Outputs:
- token_loss: float32 [1536], P(('dp', 'vocab'))
- mean_loss: float32 [], replicated
The draws below stay inside these ranges and needn't reach their ends.
All inputs are finite; a program needn't handle non-finite values.
Results may differ from the reference program's by a relative error of at most 0.00055.
Values may be sent and summed in bfloat16 or wider, within the bound.
No kernel may reach another device: no remote copies, remote signals or barrier semaphores. Data moves between devices by JAX's collectives and lax.ppermute only.
A program may use at most 64 MiB of HBM per device.

```python
import math
import jax
import jax.numpy as jnp
from jax import lax

D = 4096
V_DEV = 256
TOKENS = 1536
V = 8192


def hidden_base(key):
    values = jax.random.truncated_normal(jax.random.fold_in(key, 11), -5.0, 5.0, (TOKENS, D), jnp.float32)
    scales = 3.0
    return values * scales


def draw_hidden(key, part):
    return hidden_base(key).astype(jnp.bfloat16)


def draw_embedding(key, part):
    limit = max(0.5, float(160 // D))
    table = jax.random.truncated_normal(jax.random.fold_in(key, 12), -5.0, 5.0, (V, D), jnp.float32) / math.sqrt(D)
    table = jnp.clip(table, -limit, limit)
    return table.astype(jnp.bfloat16)


def with_ends(values, stream_key, least, high):
    longest = values.shape.index(max(values.shape))
    spots = []
    for shift in (0, 1):
        where = [jax.random.randint(jax.random.fold_in(stream_key, axis), (), 0, length) for axis, length in enumerate(values.shape)]
        where[longest] = (where[longest] + shift) % values.shape[longest]
        spots.append(tuple(where))
    return values.at[spots[0]].set(least).at[spots[1]].set(high)


def setup_inputs(seed: int = 0) -> dict:
    seeds = jax.random.split(jax.random.key(seed), 4)
    return {
        "hidden": draw_hidden(jax.random.fold_in(seeds[3], 71), 0),
        "embedding": draw_embedding(jax.random.fold_in(seeds[3], 71), 0),
        "targets": with_ends(jax.random.randint(seeds[2], (TOKENS,), 0, V), jax.random.fold_in(seeds[2], 1), 0, V - 1).astype(jnp.int32),
    }


def reference(hidden, embedding, targets):
    block_size = V_DEV * 16
    block_count = V // block_size
    blocks = embedding.reshape(block_count, block_size, D)
    offsets = jnp.arange(block_count, dtype=jnp.int32) * block_size
    columns = jnp.arange(block_size, dtype=jnp.int32)

    def advance(running, inputs):
        maxima, totals, picked = running
        weights, offset = inputs
        logits = lax.dot_general(hidden, weights, (((1,), (1,)), ((), ())), preferred_element_type=jnp.float32)
        block_max = jnp.max(logits, axis=1)
        newest = jnp.maximum(maxima, block_max)
        totals = totals * jnp.exp(maxima - newest) + jnp.sum(jnp.exp(logits - newest[:, None]), axis=1)
        matches = (targets[:, None] - offset) == columns[None, :]
        picked = picked + jnp.sum(jnp.where(matches, logits, jnp.zeros_like(logits)), axis=1)
        return (newest, totals, picked), block_max

    starting = (jnp.full((TOKENS,), -1e30, jnp.float32), jnp.zeros((TOKENS,), jnp.float32), jnp.zeros((TOKENS,), jnp.float32))
    (maxima, totals, picked), unused = lax.scan(advance, starting, (blocks, offsets))
    token_loss = maxima + jnp.log(totals) - picked
    mean_loss = jnp.sum(token_loss) / TOKENS
    return token_loss, mean_loss
```

```python
import functools
import random

import jax
import jax.numpy as jnp
from jax import lax
from jax.experimental import pallas as pl
from jax.experimental.pallas import tpu as pltpu
from jax.sharding import Mesh, PartitionSpec as P

AXES = ("dp", "ring", "core")


def plus(at, step, dims):
    return tuple((a + s) % n for a, s, n in zip(at, step, dims))


def minus(at, step, dims):
    return tuple((a - s) % n for a, s, n in zip(at, step, dims))


def hops_of(dims):
    out = []
    for k, n in enumerate(dims):
        for way in sorted({1 % n, -1 % n} - {0}):
            out.append((k, tuple(way if i == k else 0 for i in range(len(dims)))))
    return out


def relay(dims, seed=13, tries=3000):
    hops = hops_of(dims)
    total = 1
    for n in dims:
        total *= n
    cap = -(-(total - 1) // len(dims))
    while True:
        rnd = random.Random(seed)
        left = [tries]

        def extend(k, steps, places, used):
            left[0] -= 1
            if left[0] < 0:
                return None
            if k == total:
                return steps, places
            recent = [{s[1 + c][0] for s in steps[-2:]} for c in (0, 1)]
            options = []
            for source in range(max(1, k - 1)):
                for even in hops:
                    if even[0] in recent[0] or used[0][even[0]] >= cap:
                        continue
                    to_even = plus(places[0][source], even[1], dims)
                    if to_even in places[0]:
                        continue
                    for odd in hops:
                        if odd[0] == even[0] or odd[0] in recent[1] or used[1][odd[0]] >= cap:
                            continue
                        to_odd = plus(places[1][source], odd[1], dims)
                        if to_odd not in places[1]:
                            options.append((source, even, odd, to_even, to_odd))
            rnd.shuffle(options)
            options.sort(key=lambda o: o[0])
            if rnd.random() < 0.5:
                rnd.shuffle(options)
            for source, even, odd, to_even, to_odd in options:
                now = [list(used[0]), list(used[1])]
                now[0][even[0]] += 1
                now[1][odd[0]] += 1
                found = extend(
                    k + 1,
                    steps + [(source, even, odd)],
                    (places[0] + [to_even], places[1] + [to_odd]),
                    now,
                )
                if found:
                    return found
            return None

        origin = [tuple(0 for _ in dims)]
        found = extend(1, [], (origin, origin), [[0] * len(dims)] * 2)
        if found:
            return found
        seed += 1


def score_kernel(count, slots, slot_ref, dev_ref, base_ref, *refs):
    blocks = refs[:count]
    mine, theirs, targets, kept, stats = refs[count:]
    tok = blocks[0].shape[0]
    rows = mine.shape[0]
    groups = stats.shape[0] // 2
    left = jnp.concatenate([b[...] for b in blocks], axis=0) if count > 1 else blocks[0][...]
    stats[...] = kept[...]
    logits = []
    for table in (mine, theirs):
        logits.append(
            lax.dot_general(
                table[...], left, (((1,), (1,)), ((), ())), preferred_element_type=jnp.float32
            )
        )
    wanted = jnp.concatenate([targets[pl.ds(dev_ref[s], 1), :] for s in slots], axis=1)
    maxima = functools.reduce(jnp.maximum, [jnp.max(x, axis=0, keepdims=True) for x in logits])
    totals = 0.0
    picked = 0.0
    ids = lax.broadcasted_iota(jnp.int32, logits[0].shape, 0)
    for k, x in enumerate(logits):
        totals += jnp.sum(jnp.exp(x - maxima), axis=0, keepdims=True)
        picked += jnp.sum(
            jnp.where(ids == wanted - base_ref[k], x, jnp.zeros_like(x)), axis=0, keepdims=True
        )
    level = maxima + jnp.log(totals)
    for i, s in enumerate(slots):
        at = slot_ref[s]
        stats[pl.ds(at, 1), :] = level[:, i * tok : (i + 1) * tok]
        stats[pl.ds(groups + at, 1), :] = picked[:, i * tok : (i + 1) * tok]


def score(slots, blocks, mine, theirs, targets, kept, slot_of, dev_of, bases):
    count = len(blocks)
    smem = pl.BlockSpec(memory_space=pltpu.SMEM)
    vmem = pl.BlockSpec(memory_space=pltpu.VMEM)
    tok, width = blocks[0].shape
    rows = mine.shape[0] * 2
    return pl.pallas_call(
        functools.partial(score_kernel, count, slots),
        out_shape=jax.ShapeDtypeStruct(kept.shape, jnp.float32),
        in_specs=[smem] * 3 + [vmem] * (count + 4),
        out_specs=vmem,
        cost_estimate=pl.CostEstimate(
            flops=2 * rows * width * tok * count,
            bytes_accessed=2 * width * (rows + tok * count),
            transcendentals=rows * tok * count,
        ),
        compiler_params=pltpu.CompilerParams(vmem_limit_bytes=24 * 1024 * 1024),
        name="score",
    )(slot_of, dev_of, bases, *blocks, mine, theirs, targets, kept)


def joined(parts):
    half = parts[0].shape[0] // 2
    levels = [p[:half] for p in parts]
    top = functools.reduce(jnp.maximum, levels)
    total = functools.reduce(jnp.add, [jnp.exp(x - top) for x in levels])
    picked = functools.reduce(jnp.add, [p[half:] for p in parts])
    return jnp.concatenate([top + jnp.log(total), picked], axis=0)


def local(mesh_sizes, dims, hidden, embedding, targets):
    dp, ring, cores = mesh_sizes
    chips = dp * ring
    tok = hidden.shape[0]
    rows = embedding.shape[0]
    chip = lax.axis_index("dp") * ring + lax.axis_index("ring")
    core = lax.axis_index("core")
    device = chip * cores + core

    strides = [1] * len(dims)
    for k in reversed(range(len(dims) - 1)):
        strides[k] = strides[k + 1] * dims[k + 1]
    spots = [tuple(i // s % n for s, n in zip(strides, dims)) for i in range(chips)]
    index = {spot: i for i, spot in enumerate(spots)}

    def moved(array, steps, swap=False):
        pairs = []
        for i, spot in enumerate(spots):
            for c in range(cores):
                to = index[plus(spot, steps[c], dims)]
                pairs.append((i * cores + c, to * cores + (cores - 1 - c if swap else c)))
        return lax.ppermute(array, AXES, pairs)

    steps, places = relay(dims)
    still = (tuple(0 for _ in dims),) * cores
    theirs = moved(embedding, still, swap=True)

    owners = jnp.array(
        [[[index[minus(spot, at, dims)] for at in places[c]] for c in range(cores)] for spot in spots],
        jnp.int32,
    )
    slot_of = owners[chip, core]
    dev_of = slot_of * cores + core
    bases = jnp.stack([device * rows, (chip * cores + (cores - 1 - core)) * rows])
    wanted = targets.reshape(chips * cores, tok)

    blocks = [hidden]
    for source, even, odd in steps:
        blocks.append(moved(blocks[source], (even[1], odd[1])))

    stats = jnp.zeros((2 * chips, tok), jnp.float32)
    batch = len(dims)
    edges = [0, 1] + list(range(1 + batch, chips, batch)) + [chips]
    for low, high in zip(edges[:-1], edges[1:]):
        slots = tuple(range(low, high))
        stats = score(
            slots, [blocks[s] for s in slots], embedding, theirs, wanted, stats, slot_of, dev_of, bases
        )

    turns = [plus(still[0], s, dims) for s in spots[1:]]
    along = [t for t in turns if sum(1 for v in t if v) == 1 and t[1]]
    across = [t for t in turns if not t[1]]
    stats = joined([stats] + [moved(stats, (t,) * cores) for t in along])
    stats = joined([stats] + [moved(stats, (t,) * cores) for t in across])
    losses = stats[:chips] - stats[chips:]
    other = moved(losses, still, swap=True)
    mean_loss = (jnp.sum(losses) + jnp.sum(other)) / (tok * chips * cores)
    token_loss = lax.dynamic_slice_in_dim(losses, chip, 1).reshape(tok)
    return token_loss, mean_loss


def gathered(hidden, embedding, targets):
    tok, rows = hidden.shape[0], embedding.shape[0]
    device = lax.axis_index(AXES)
    tokens = lax.all_gather(hidden, AXES, axis=0, tiled=True)
    logits = lax.dot_general(
        tokens, embedding, (((1,), (1,)), ((), ())), preferred_element_type=jnp.float32
    )
    ids = device * rows + jnp.arange(rows, dtype=jnp.int32)
    maxima = lax.pmax(jnp.max(logits, axis=1), AXES)
    totals = jnp.sum(jnp.exp(logits - maxima[:, None]), axis=1)
    picked = jnp.sum(
        jnp.where(targets[:, None] == ids[None, :], logits, jnp.zeros_like(logits)), axis=1
    )
    totals, picked = lax.psum((totals, picked), AXES)
    losses = maxima + jnp.log(totals) - picked
    token_loss = lax.dynamic_slice_in_dim(losses, device * tok, tok)
    return token_loss, jnp.sum(losses) / losses.shape[0]


def solution(mesh):
    dp, vocab = mesh.shape["dp"], mesh.shape["vocab"]
    sizes = (dp, vocab // 2, 2)
    dims = (dp, vocab // 4, 2)
    fine = Mesh(mesh.devices.reshape(sizes), AXES)
    body = functools.partial(local, sizes, dims) if dp * vocab <= 64 else gathered
    return jax.shard_map(
        body,
        mesh=fine,
        in_specs=(P(AXES, None), P(AXES, None), P()),
        out_specs=(P(AXES), P()),
        check_vma=False,
    )
```

```python
import functools
import math
import random

import jax
import jax.numpy as jnp
from jax import lax
from jax.experimental import pallas as pl
from jax.experimental.pallas import tpu as pltpu
from jax.sharding import Mesh, PartitionSpec as P


AXES = ("dp", "ring", "core")
SEED = 6000647


def plus(at, step, dims):
    return tuple((a + s) % n for a, s, n in zip(at, step, dims))


def minus(at, step, dims):
    return tuple((a - s) % n for a, s, n in zip(at, step, dims))


def hops_of(dims):
    out = []
    for k, n in enumerate(dims):
        for way in sorted({1 % n, -1 % n} - {0}):
            out.append((k, tuple(way if i == k else 0 for i in range(len(dims)))))
    return out


def attempt(dims, seed, tries):
    hops = hops_of(dims)
    total = math.prod(dims)
    cap = -(-(total - 1) // len(dims))
    origin = [tuple(0 for _ in dims)]
    rnd = random.Random(seed)
    lag = rnd.choice((1, 2, 2))
    apart = rnd.random() < 0.7
    left = [tries]

    def extend(k, steps, places, used):
        left[0] -= 1
        if left[0] < 0:
            return None
        if k == total:
            return steps, places
        options = []
        for source in range(max(1, k - lag + 1)):
            for even in hops:
                to_even = plus(places[0][source], even[1], dims)
                if used[0][even[0]] >= cap or to_even in places[0]:
                    continue
                for odd in hops:
                    to_odd = plus(places[1][source], odd[1], dims)
                    if apart and odd[0] == even[0]:
                        continue
                    if used[1][odd[0]] >= cap or to_odd in places[1]:
                        continue
                    if steps and any(h[0] == p[0] for h, p in zip((even, odd), steps[-1][1:])):
                        continue
                    options.append((source, even, odd, to_even, to_odd))
        rnd.shuffle(options)
        options.sort(key=lambda o: o[0] + rnd.random() * 2 * len(dims))
        for source, even, odd, to_even, to_odd in options[:4]:
            now = [list(used[0]), list(used[1])]
            now[0][even[0]] += 1
            now[1][odd[0]] += 1
            found = extend(
                k + 1,
                steps + [(source, even, odd)],
                (places[0] + [to_even], places[1] + [to_odd]),
                now,
            )
            if found:
                return found
        return None

    return extend(1, [], (origin, origin), [[0] * len(dims)] * 2)


def relay(dims, seed=SEED, tries=400):
    while True:
        found = attempt(dims, seed, tries)
        if found:
            return found
        seed += 1


def score_kernel(count, slots, slot_ref, dev_ref, base_ref, *refs):
    blocks = refs[:count]
    mine, theirs, targets, kept, stats = refs[count:]
    tok = blocks[0].shape[0]
    groups = stats.shape[0] // 2
    left = jnp.concatenate([b[...] for b in blocks], axis=0) if count > 1 else blocks[0][...]
    stats[...] = kept[...]
    logits = []
    for table in (mine, theirs):
        logits.append(
            lax.dot_general(
                table[...], left, (((1,), (1,)), ((), ())), preferred_element_type=jnp.float32
            )
        )
    wanted = jnp.concatenate([targets[pl.ds(dev_ref[s], 1), :] for s in slots], axis=1)
    maxima = functools.reduce(jnp.maximum, [jnp.max(x, axis=0, keepdims=True) for x in logits])
    totals = 0.0
    picked = 0.0
    ids = lax.broadcasted_iota(jnp.int32, logits[0].shape, 0)
    for k, x in enumerate(logits):
        totals += jnp.sum(jnp.exp(x - maxima), axis=0, keepdims=True)
        picked += jnp.sum(
            jnp.where(ids == wanted - base_ref[k], x, jnp.zeros_like(x)), axis=0, keepdims=True
        )
    level = maxima + jnp.log(totals)
    for i, s in enumerate(slots):
        at = slot_ref[s]
        stats[pl.ds(at, 1), :] = level[:, i * tok : (i + 1) * tok]
        stats[pl.ds(groups + at, 1), :] = picked[:, i * tok : (i + 1) * tok]


def score(slots, blocks, mine, theirs, targets, kept, slot_of, dev_of, bases):
    count = len(blocks)
    smem = pl.BlockSpec(memory_space=pltpu.SMEM)
    vmem = pl.BlockSpec(memory_space=pltpu.VMEM)
    tok, width = blocks[0].shape
    rows = mine.shape[0] * 2
    return pl.pallas_call(
        functools.partial(score_kernel, count, slots),
        out_shape=jax.ShapeDtypeStruct(kept.shape, jnp.float32),
        in_specs=[smem] * 3 + [vmem] * (count + 4),
        out_specs=vmem,
        cost_estimate=pl.CostEstimate(
            flops=2 * rows * width * tok * count,
            bytes_accessed=2 * width * (rows + tok * count),
            transcendentals=rows * tok * count,
        ),
        compiler_params=pltpu.CompilerParams(vmem_limit_bytes=24 * 1024 * 1024),
        name="score",
    )(slot_of, dev_of, bases, *blocks, mine, theirs, targets, kept)


def batches_of(dims):
    total = math.prod(dims)
    last = total - len(dims)
    edges = (0, (last + 1) // 2, last, total)
    return [tuple(range(low, high)) for low, high in zip(edges[:-1], edges[1:])]


def joined(parts):
    half = parts[0].shape[0] // 2
    levels = [p[:half] for p in parts]
    top = functools.reduce(jnp.maximum, levels)
    total = functools.reduce(jnp.add, [jnp.exp(x - top) for x in levels])
    picked = functools.reduce(jnp.add, [p[half:] for p in parts])
    return jnp.concatenate([top + jnp.log(total), picked], axis=0)


def local(mesh_sizes, dims, hidden, embedding, targets):
    return share(mesh_sizes, dims, hidden, embedding, targets)


def share(mesh_sizes, dims, hidden, embedding, targets):
    dp, ring, cores = mesh_sizes
    chips = dp * ring
    tok = hidden.shape[0]
    rows = embedding.shape[0]
    chip = lax.axis_index("dp") * ring + lax.axis_index("ring")
    core = lax.axis_index("core")
    device = chip * cores + core

    strides = [1] * len(dims)
    for k in reversed(range(len(dims) - 1)):
        strides[k] = strides[k + 1] * dims[k + 1]
    spots = [tuple(i // s % n for s, n in zip(strides, dims)) for i in range(chips)]
    index = {spot: i for i, spot in enumerate(spots)}

    def moved(array, steps, swap=False):
        pairs = []
        for i, spot in enumerate(spots):
            for c in range(cores):
                to = index[plus(spot, steps[c], dims)]
                pairs.append((i * cores + c, to * cores + (cores - 1 - c if swap else c)))
        return lax.ppermute(array, AXES, pairs)

    steps, places = relay(dims)
    still = (tuple(0 for _ in dims),) * cores
    theirs = moved(embedding, still, swap=True)

    owners = jnp.array(
        [[[index[minus(spot, at, dims)] for at in places[c]] for c in range(cores)] for spot in spots],
        jnp.int32,
    )
    slot_of = owners[chip, core]
    dev_of = slot_of * cores + core
    bases = jnp.stack([device * rows, (chip * cores + (cores - 1 - core)) * rows])
    wanted = targets.reshape(chips * cores, tok)

    blocks = [hidden]
    for k, (source, even, odd) in enumerate(steps, 1):
        blocks.append(moved(blocks[source], (even[1], odd[1])))

    stats = jnp.zeros((2 * chips, tok), jnp.float32)
    for slots in batches_of(dims):
        stats = score(
            slots, [blocks[s] for s in slots], embedding, theirs, wanted, stats, slot_of, dev_of, bases
        )

    turns = [plus(still[0], s, dims) for s in spots[1:]]
    along = [t for t in turns if sum(1 for v in t if v) == 1 and t[1]]
    across = [t for t in turns if not t[1]]
    stats = joined([stats] + [moved(stats, (t,) * cores) for t in along])
    stats = joined([stats] + [moved(stats, (t,) * cores) for t in across])
    losses = stats[:chips] - stats[chips:]
    other = moved(losses, still, swap=True)
    mean_loss = (jnp.sum(losses) + jnp.sum(other)) / (tok * chips * cores)
    token_loss = lax.dynamic_slice_in_dim(losses, chip, 1).reshape(tok)
    return token_loss, mean_loss


def gathered(hidden, embedding, targets):
    tok, rows = hidden.shape[0], embedding.shape[0]
    device = lax.axis_index(AXES)
    tokens = lax.all_gather(hidden, AXES, axis=0, tiled=True)
    logits = lax.dot_general(
        tokens, embedding, (((1,), (1,)), ((), ())), preferred_element_type=jnp.float32
    )
    ids = device * rows + jnp.arange(rows, dtype=jnp.int32)
    maxima = lax.pmax(jnp.max(logits, axis=1), AXES)
    totals = jnp.sum(jnp.exp(logits - maxima[:, None]), axis=1)
    picked = jnp.sum(
        jnp.where(targets[:, None] == ids[None, :], logits, jnp.zeros_like(logits)), axis=1
    )
    totals, picked = lax.psum((totals, picked), AXES)
    losses = maxima + jnp.log(totals) - picked
    token_loss = lax.dynamic_slice_in_dim(losses, device * tok, tok)
    return token_loss, jnp.sum(losses) / losses.shape[0]


def solution(mesh):
    dp, vocab = mesh.shape["dp"], mesh.shape["vocab"]
    sizes = (dp, vocab // 2, 2)
    dims = (dp, vocab // 4, 2)
    fine = Mesh(mesh.devices.reshape(sizes), AXES)
    few = dp * vocab <= 64
    return jax.shard_map(
        functools.partial(local, sizes, dims) if few else gathered,
        mesh=fine,
        in_specs=(P(AXES, None), P(AXES, None), P()),
        out_specs=(P(AXES), P()),
        check_vma=False,
    )
```

```python
import functools
import math
import random

import jax
import jax.numpy as jnp
from jax import lax
from jax.experimental import pallas as pl
from jax.experimental.pallas import tpu as pltpu
from jax.sharding import Mesh, PartitionSpec as P


AXES = ("dp", "ring", "core")
SEED = 2000322
PIECES = 4
VMEM_MIB = 24


def across(at, step):
    return tuple(a ^ s for a, s in zip(at, step))


def hops_of(dims):
    out = []
    for k, n in enumerate(dims):
        way = 1
        while way < n:
            out.append((k, tuple(way if i == k else 0 for i in range(len(dims)))))
            way = 2 * way + 1
    return out


def attempt(dims, seed, tries):
    hops = hops_of(dims)
    total = math.prod(dims)
    cap = -(-(total - 1) // len(dims))
    origin = [tuple(0 for _ in dims)]
    rnd = random.Random(seed)
    lag = rnd.choice((1, 2, 2))
    apart = rnd.random() < 0.7
    left = [tries]

    def extend(k, steps, places, used):
        left[0] -= 1
        if left[0] < 0:
            return None
        if k == total:
            return steps, places
        options = []
        for source in range(max(1, k - lag + 1)):
            for even in hops:
                to_even = across(places[0][source], even[1])
                if used[0][even[0]] >= cap or to_even in places[0]:
                    continue
                for odd in hops:
                    to_odd = across(places[1][source], odd[1])
                    if apart and odd[0] == even[0]:
                        continue
                    if used[1][odd[0]] >= cap or to_odd in places[1]:
                        continue
                    if steps and any(h[0] == p[0] for h, p in zip((even, odd), steps[-1][1:])):
                        continue
                    options.append((source, even, odd, to_even, to_odd))
        rnd.shuffle(options)
        options.sort(key=lambda o: o[0] + rnd.random() * 2 * len(dims))
        for source, even, odd, to_even, to_odd in options[:4]:
            now = [list(used[0]), list(used[1])]
            now[0][even[0]] += 1
            now[1][odd[0]] += 1
            found = extend(
                k + 1,
                steps + [(source, even, odd)],
                (places[0] + [to_even], places[1] + [to_odd]),
                now,
            )
            if found:
                return found
        return None

    return extend(1, [], (origin, origin), [[0] * len(dims)] * 2)


def relay(dims, seed=SEED, tries=400):
    while True:
        found = attempt(dims, seed, tries)
        if found:
            return found
        seed += 1


def score_kernel(count, slots, slot_ref, dev_ref, base_ref, *refs):
    blocks = refs[:count]
    mine, theirs, targets, kept, stats = refs[count:]
    tok = blocks[0].shape[0]
    groups = stats.shape[0] // 2
    left = jnp.concatenate([b[...] for b in blocks], axis=0) if count > 1 else blocks[0][...]
    stats[...] = kept[...]
    logits = []
    for table in (mine, theirs):
        logits.append(
            lax.dot_general(
                table[...], left, (((1,), (1,)), ((), ())), preferred_element_type=jnp.float32
            )
        )
    wanted = jnp.concatenate([targets[pl.ds(dev_ref[s], 1), :] for s in slots], axis=1)
    maxima = functools.reduce(jnp.maximum, [jnp.max(x, axis=0, keepdims=True) for x in logits])
    totals = 0.0
    picked = 0.0
    ids = lax.broadcasted_iota(jnp.int32, logits[0].shape, 0)
    for k, x in enumerate(logits):
        totals += jnp.sum(jnp.exp(x - maxima), axis=0, keepdims=True)
        picked += jnp.sum(
            jnp.where(ids == wanted - base_ref[k], x, jnp.zeros_like(x)), axis=0, keepdims=True
        )
    level = maxima + jnp.log(totals)
    for i, s in enumerate(slots):
        at = slot_ref[s]
        stats[pl.ds(at, 1), :] = level[:, i * tok : (i + 1) * tok]
        stats[pl.ds(groups + at, 1), :] = picked[:, i * tok : (i + 1) * tok]


def score(slots, blocks, mine, theirs, targets, kept, slot_of, dev_of, bases):
    count = len(blocks)
    smem = pl.BlockSpec(memory_space=pltpu.SMEM)
    vmem = pl.BlockSpec(memory_space=pltpu.VMEM)
    tok, width = blocks[0].shape
    rows = mine.shape[0] * 2
    return pl.pallas_call(
        functools.partial(score_kernel, count, slots),
        out_shape=jax.ShapeDtypeStruct(kept.shape, jnp.float32),
        in_specs=[smem] * 3 + [vmem] * (count + 4),
        out_specs=vmem,
        cost_estimate=pl.CostEstimate(
            flops=2 * rows * width * tok * count,
            bytes_accessed=2 * width * (rows + tok * count),
            transcendentals=rows * tok * count,
        ),
        compiler_params=pltpu.CompilerParams(vmem_limit_bytes=VMEM_MIB * 2**20),
        name="score",
    )(slot_of, dev_of, bases, *blocks, mine, theirs, targets, kept)


def batches_of(dims):
    total = math.prod(dims)
    early = total - len(dims)
    edges = [early * i // PIECES for i in range(PIECES + 1)] + [total]
    return [tuple(range(low, high)) for low, high in zip(edges[:-1], edges[1:])]


def tree(op, parts):
    while len(parts) > 1:
        parts = [op(*parts[i : i + 2]) if i + 1 < len(parts) else parts[i] for i in range(0, len(parts), 2)]
    return parts[0]


def joined(parts):
    half = parts[0].shape[0] // 2
    levels = [p[:half] for p in parts]
    top = tree(jnp.maximum, levels)
    total = tree(jnp.add, [jnp.exp(x - top) for x in levels])
    return top + jnp.log(total), tree(jnp.add, [p[half:] for p in parts])


def finish_kernel(row_ref, mine, theirs, token_loss, mean_loss):
    token_loss[...] = mine[pl.ds(row_ref[0], 1), :]
    count = mine.shape[0] * mine.shape[1] * 2
    total = jnp.sum(mine[...], keepdims=True) + jnp.sum(theirs[...], keepdims=True)
    mean_loss[...] = total / count


def finish(row, mine, theirs):
    vmem = pl.BlockSpec(memory_space=pltpu.VMEM)
    token_loss, mean_loss = pl.pallas_call(
        finish_kernel,
        out_shape=(
            jax.ShapeDtypeStruct((1, mine.shape[1]), jnp.float32),
            jax.ShapeDtypeStruct((1, 1), jnp.float32),
        ),
        in_specs=[pl.BlockSpec(memory_space=pltpu.SMEM), vmem, vmem],
        out_specs=(vmem, vmem),
        compiler_params=pltpu.CompilerParams(vmem_limit_bytes=VMEM_MIB * 2**20),
        name="finish",
    )(row.reshape(1), mine, theirs)
    return token_loss.reshape(mine.shape[1]), mean_loss.reshape(())


def local(mesh_sizes, dims, hidden, embedding, targets):
    return share(mesh_sizes, dims, hidden, embedding, targets)


def share(mesh_sizes, dims, hidden, embedding, targets):
    dp, ring, cores = mesh_sizes
    chips = dp * ring
    tok = hidden.shape[0]
    rows = embedding.shape[0]
    chip = lax.axis_index("dp") * ring + lax.axis_index("ring")
    core = lax.axis_index("core")
    device = chip * cores + core

    strides = [1] * len(dims)
    for k in reversed(range(len(dims) - 1)):
        strides[k] = strides[k + 1] * dims[k + 1]
    spots = [tuple(i // s % n for s, n in zip(strides, dims)) for i in range(chips)]
    index = {spot: i for i, spot in enumerate(spots)}

    def moved(array, steps, swap=False):
        pairs = []
        for i, spot in enumerate(spots):
            for c in range(cores):
                to = index[across(spot, steps[c])]
                pairs.append((i * cores + c, to * cores + (cores - 1 - c if swap else c)))
        return lax.ppermute(array, AXES, pairs)

    steps, places = relay(dims)
    still = (tuple(0 for _ in dims),) * cores
    theirs = moved(embedding, still, swap=True)

    owners = jnp.array(
        [[[index[across(spot, at)] for at in places[c]] for c in range(cores)] for spot in spots],
        jnp.int32,
    )
    slot_of = owners[chip, core]
    dev_of = slot_of * cores + core
    bases = jnp.stack([device * rows, (chip * cores + (cores - 1 - core)) * rows])
    wanted = targets.reshape(chips * cores, tok)

    blocks = [hidden]
    for k, (source, even, odd) in enumerate(steps, 1):
        blocks.append(moved(blocks[source], (even[1], odd[1])))

    stats = jnp.zeros((2 * chips, tok), jnp.float32)
    for slots in batches_of(dims):
        stats = score(
            slots, [blocks[s] for s in slots], embedding, theirs, wanted, stats, slot_of, dev_of, bases
        )

    long = dims.index(max(dims))
    turns = [
        [t for t in spots[1:] if not any(v for k, v in enumerate(t) if k != long)],
        [t for t in spots[1:] if not t[long]],
    ]
    for stage in turns:
        level, picked = joined([stats] + [moved(stats, (t,) * cores) for t in stage])
        stats = jnp.concatenate([level, picked], axis=0)
    losses = level - picked
    return finish(chip, losses, moved(losses, still, swap=True))


def gathered(hidden, embedding, targets):
    tok, rows = hidden.shape[0], embedding.shape[0]
    device = lax.axis_index(AXES)
    tokens = lax.all_gather(hidden, AXES, axis=0, tiled=True)
    logits = lax.dot_general(
        tokens, embedding, (((1,), (1,)), ((), ())), preferred_element_type=jnp.float32
    )
    ids = device * rows + jnp.arange(rows, dtype=jnp.int32)
    maxima = lax.pmax(jnp.max(logits, axis=1), AXES)
    totals = jnp.sum(jnp.exp(logits - maxima[:, None]), axis=1)
    picked = jnp.sum(
        jnp.where(targets[:, None] == ids[None, :], logits, jnp.zeros_like(logits)), axis=1
    )
    totals, picked = lax.psum((totals, picked), AXES)
    losses = maxima + jnp.log(totals) - picked
    token_loss = lax.dynamic_slice_in_dim(losses, device * tok, tok)
    return token_loss, jnp.sum(losses) / losses.shape[0]


def solution(mesh):
    dp, vocab = mesh.shape["dp"], mesh.shape["vocab"]
    sizes = (dp, vocab // 2, 2)
    dims = (dp, vocab // 4, 2)
    fine = Mesh(mesh.devices.reshape(sizes), AXES)
    few = dp * vocab <= 64
    return jax.shard_map(
        functools.partial(local, sizes, dims) if few else gathered,
        mesh=fine,
        in_specs=(P(AXES, None), P(AXES, None), P()),
        out_specs=(P(AXES), P()),
        check_vma=False,
    )
```

```python
import functools
import itertools
import math
import random

import jax
import jax.numpy as jnp
from jax import lax
from jax.experimental import pallas as pl
from jax.experimental.pallas import tpu as pltpu
from jax.sharding import Mesh, PartitionSpec as P


AXES = ("dp", "ring", "core")
ORDER = ((0, 3, 1), (0, 4, 0), (0, 0, 4), (1, 1, 3), (1, 4, 0), (1, 0, 4), (3, 4, 0), (2, 1, 3), (4, 4, 0), (4, 0, 4), (3, 1, 3), (8, 4, 0), (6, 4, 0), (7, 1, 3), (9, 0, 4))
PIECES = 4
VMEM_MIB = 24


def across(at, step):
    return tuple(a ^ s for a, s in zip(at, step))


def hops_of(dims):
    out = []
    for k, n in enumerate(dims):
        for way in range(1, n):
            out.append((k, tuple(way if i == k else 0 for i in range(len(dims)))))
    return out


def attempt(dims, seed, tries):
    hops = hops_of(dims)
    total = math.prod(dims)
    cap = -(-(total - 1) // len(dims))
    origin = [tuple(0 for _ in dims)]
    rnd = random.Random(seed)
    lag = rnd.choice((1, 2, 2))
    apart = rnd.random() < 0.7
    left = [tries]

    def extend(k, steps, places, used):
        left[0] -= 1
        if left[0] < 0:
            return None
        if k == total:
            return steps, places
        options = []
        for source in range(max(1, k - lag + 1)):
            for even in hops:
                to_even = across(places[0][source], even[1])
                if used[0][even[0]] >= cap or to_even in places[0]:
                    continue
                for odd in hops:
                    to_odd = across(places[1][source], odd[1])
                    if apart and odd[0] == even[0]:
                        continue
                    if used[1][odd[0]] >= cap or to_odd in places[1]:
                        continue
                    if steps and any(h[0] == p[0] for h, p in zip((even, odd), steps[-1][1:])):
                        continue
                    options.append((source, even, odd, to_even, to_odd))
        rnd.shuffle(options)
        options.sort(key=lambda o: o[0] + rnd.random() * 2 * len(dims))
        for source, even, odd, to_even, to_odd in options[:4]:
            now = [list(used[0]), list(used[1])]
            now[0][even[0]] += 1
            now[1][odd[0]] += 1
            found = extend(
                k + 1,
                steps + [(source, even, odd)],
                (places[0] + [to_even], places[1] + [to_odd]),
                now,
            )
            if found:
                return found
        return None

    return extend(1, [], (origin, origin), [[0] * len(dims)] * 2)


def placed(dims, order):
    hops = hops_of(dims)
    steps, places = [], ([tuple(0 for _ in dims)], [tuple(0 for _ in dims)])
    for source, even, odd in order:
        if max(even, odd) >= len(hops):
            return None
        steps.append((source, hops[even], hops[odd]))
        for core, (_, way) in enumerate(steps[-1][1:]):
            places[core].append(across(places[core][source], way))
    everywhere = set(itertools.product(*[range(n) for n in dims]))
    if any(len(p) != len(everywhere) or set(p) != everywhere for p in places):
        return None
    return steps, places


def relay(dims, tries=400):
    found, seed = placed(dims, ORDER), 0
    while not found:
        found, seed = attempt(dims, seed, tries), seed + 1
    return found


def score_kernel(count, slots, slot_ref, dev_ref, base_ref, *refs):
    blocks = refs[:count]
    mine, theirs, targets, kept, stats = refs[count:]
    tok = blocks[0].shape[0]
    groups = stats.shape[0] // 2
    left = jnp.concatenate([b[...] for b in blocks], axis=0) if count > 1 else blocks[0][...]
    stats[...] = kept[...]
    logits = []
    for table in (mine, theirs):
        logits.append(
            lax.dot_general(
                table[...], left, (((1,), (1,)), ((), ())), preferred_element_type=jnp.float32
            )
        )
    wanted = jnp.concatenate([targets[pl.ds(dev_ref[s], 1), :] for s in slots], axis=1)
    maxima = functools.reduce(jnp.maximum, [jnp.max(x, axis=0, keepdims=True) for x in logits])
    totals = 0.0
    picked = 0.0
    ids = lax.broadcasted_iota(jnp.int32, logits[0].shape, 0)
    for k, x in enumerate(logits):
        totals += jnp.sum(jnp.exp(x - maxima), axis=0, keepdims=True)
        picked += jnp.sum(
            jnp.where(ids == wanted - base_ref[k], x, jnp.zeros_like(x)), axis=0, keepdims=True
        )
    level = maxima + jnp.log(totals)
    for i, s in enumerate(slots):
        at = slot_ref[s]
        stats[pl.ds(at, 1), :] = level[:, i * tok : (i + 1) * tok]
        stats[pl.ds(groups + at, 1), :] = picked[:, i * tok : (i + 1) * tok]


def score(slots, blocks, mine, theirs, targets, kept, slot_of, dev_of, bases):
    count = len(blocks)
    smem = pl.BlockSpec(memory_space=pltpu.SMEM)
    vmem = pl.BlockSpec(memory_space=pltpu.VMEM)
    tok, width = blocks[0].shape
    rows = mine.shape[0] * 2
    return pl.pallas_call(
        functools.partial(score_kernel, count, slots),
        out_shape=jax.ShapeDtypeStruct(kept.shape, jnp.float32),
        in_specs=[smem] * 3 + [vmem] * (count + 4),
        out_specs=vmem,
        cost_estimate=pl.CostEstimate(
            flops=2 * rows * width * tok * count,
            bytes_accessed=2 * width * (rows + tok * count),
            transcendentals=rows * tok * count,
        ),
        compiler_params=pltpu.CompilerParams(vmem_limit_bytes=VMEM_MIB * 2**20),
        name="score",
    )(slot_of, dev_of, bases, *blocks, mine, theirs, targets, kept)


def batches_of(dims):
    total = math.prod(dims)
    early = total - len(dims)
    edges = [early * i // PIECES for i in range(PIECES + 1)] + [total]
    return [tuple(range(low, high)) for low, high in zip(edges[:-1], edges[1:])]


def tree(op, parts):
    while len(parts) > 1:
        parts = [op(*parts[i : i + 2]) if i + 1 < len(parts) else parts[i] for i in range(0, len(parts), 2)]
    return parts[0]


def joined(parts):
    half = parts[0].shape[0] // 2
    levels = [p[:half] for p in parts]
    top = tree(jnp.maximum, levels)
    total = tree(jnp.add, [jnp.exp(x - top) for x in levels])
    return top + jnp.log(total), tree(jnp.add, [p[half:] for p in parts])


def finish_kernel(row_ref, mine, theirs, token_loss, mean_loss):
    token_loss[...] = mine[pl.ds(row_ref[0], 1), :]
    count = mine.shape[0] * mine.shape[1] * 2
    total = jnp.sum(mine[...], keepdims=True) + jnp.sum(theirs[...], keepdims=True)
    mean_loss[...] = total / count


def finish(row, mine, theirs):
    vmem = pl.BlockSpec(memory_space=pltpu.VMEM)
    token_loss, mean_loss = pl.pallas_call(
        finish_kernel,
        out_shape=(
            jax.ShapeDtypeStruct((1, mine.shape[1]), jnp.float32),
            jax.ShapeDtypeStruct((1, 1), jnp.float32),
        ),
        in_specs=[pl.BlockSpec(memory_space=pltpu.SMEM), vmem, vmem],
        out_specs=(vmem, vmem),
        compiler_params=pltpu.CompilerParams(vmem_limit_bytes=VMEM_MIB * 2**20),
        name="finish",
    )(row.reshape(1), mine, theirs)
    return token_loss.reshape(mine.shape[1]), mean_loss.reshape(())


def local(mesh_sizes, dims, hidden, embedding, targets):
    return share(mesh_sizes, dims, hidden, embedding, targets)


def share(mesh_sizes, dims, hidden, embedding, targets):
    dp, ring, cores = mesh_sizes
    chips = dp * ring
    tok = hidden.shape[0]
    rows = embedding.shape[0]
    chip = lax.axis_index("dp") * ring + lax.axis_index("ring")
    core = lax.axis_index("core")
    device = chip * cores + core

    strides = [1] * len(dims)
    for k in reversed(range(len(dims) - 1)):
        strides[k] = strides[k + 1] * dims[k + 1]
    spots = [tuple(i // s % n for s, n in zip(strides, dims)) for i in range(chips)]
    index = {spot: i for i, spot in enumerate(spots)}

    def moved(array, steps, swap=False):
        pairs = []
        for i, spot in enumerate(spots):
            for c in range(cores):
                to = index[across(spot, steps[c])]
                pairs.append((i * cores + c, to * cores + (cores - 1 - c if swap else c)))
        return lax.ppermute(array, AXES, pairs)

    steps, places = relay(dims)
    still = (tuple(0 for _ in dims),) * cores
    theirs = moved(embedding, still, swap=True)

    owners = jnp.array(
        [[[index[across(spot, at)] for at in places[c]] for c in range(cores)] for spot in spots],
        jnp.int32,
    )
    slot_of = owners[chip, core]
    dev_of = slot_of * cores + core
    bases = jnp.stack([device * rows, (chip * cores + (cores - 1 - core)) * rows])
    wanted = targets.reshape(chips * cores, tok)

    blocks = [hidden]
    for k, (source, even, odd) in enumerate(steps, 1):
        blocks.append(moved(blocks[source], (even[1], odd[1])))

    stats = jnp.zeros((2 * chips, tok), jnp.float32)
    for slots in batches_of(dims):
        stats = score(
            slots, [blocks[s] for s in slots], embedding, theirs, wanted, stats, slot_of, dev_of, bases
        )

    long = dims.index(max(dims))
    turns = [
        [t for t in spots[1:] if not any(v for k, v in enumerate(t) if k != long)],
        [t for t in spots[1:] if not t[long]],
    ]
    for stage in turns:
        level, picked = joined([stats] + [moved(stats, (t,) * cores) for t in stage])
        stats = jnp.concatenate([level, picked], axis=0)
    losses = level - picked
    return finish(chip, losses, moved(losses, still, swap=True))


def gathered(hidden, embedding, targets):
    tok, rows = hidden.shape[0], embedding.shape[0]
    device = lax.axis_index(AXES)
    tokens = lax.all_gather(hidden, AXES, axis=0, tiled=True)
    logits = lax.dot_general(
        tokens, embedding, (((1,), (1,)), ((), ())), preferred_element_type=jnp.float32
    )
    ids = device * rows + jnp.arange(rows, dtype=jnp.int32)
    maxima = lax.pmax(jnp.max(logits, axis=1), AXES)
    totals = jnp.sum(jnp.exp(logits - maxima[:, None]), axis=1)
    picked = jnp.sum(
        jnp.where(targets[:, None] == ids[None, :], logits, jnp.zeros_like(logits)), axis=1
    )
    totals, picked = lax.psum((totals, picked), AXES)
    losses = maxima + jnp.log(totals) - picked
    token_loss = lax.dynamic_slice_in_dim(losses, device * tok, tok)
    return token_loss, jnp.sum(losses) / losses.shape[0]


def solution(mesh):
    dp, vocab = mesh.shape["dp"], mesh.shape["vocab"]
    sizes = (dp, vocab // 2, 2)
    dims = (dp, vocab // 4, 2)
    fine = Mesh(mesh.devices.reshape(sizes), AXES)
    few = dp * vocab <= 64
    return jax.shard_map(
        functools.partial(local, sizes, dims) if few else gathered,
        mesh=fine,
        in_specs=(P(AXES, None), P(AXES, None), P()),
        out_specs=(P(AXES), P()),
        check_vma=False,
    )
```

```python
import functools
import itertools
import math
import random

import jax
import jax.numpy as jnp
from jax import lax
from jax.experimental import pallas as pl
from jax.experimental.pallas import tpu as pltpu
from jax.sharding import Mesh, PartitionSpec as P


AXES = ("dp", "ring", "core")
ORDER = ((0, 3, 1), (0, 4, 0), (0, 0, 4), (1, 1, 3), (1, 0, 4), (1, 4, 0), (2, 0, 4), (0, 1, 3), (4, 4, 0), (4, 0, 4), (2, 1, 3), (8, 0, 4), (6, 0, 4), (7, 1, 3), (10, 4, 0))
PIECES = 4
VMEM_MIB = 24


def across(at, step):
    return tuple(a ^ s for a, s in zip(at, step))


def hops_of(dims):
    out = []
    for k, n in enumerate(dims):
        for way in range(1, n):
            out.append((k, tuple(way if i == k else 0 for i in range(len(dims)))))
    return out


def attempt(dims, seed, tries):
    hops = hops_of(dims)
    total = math.prod(dims)
    cap = -(-(total - 1) // len(dims))
    origin = [tuple(0 for _ in dims)]
    rnd = random.Random(seed)
    lag = rnd.choice((1, 2, 2))
    apart = rnd.random() < 0.7
    left = [tries]

    def extend(k, steps, places, used):
        left[0] -= 1
        if left[0] < 0:
            return None
        if k == total:
            return steps, places
        options = []
        for source in range(max(1, k - lag + 1)):
            for even in hops:
                to_even = across(places[0][source], even[1])
                if used[0][even[0]] >= cap or to_even in places[0]:
                    continue
                for odd in hops:
                    to_odd = across(places[1][source], odd[1])
                    if apart and odd[0] == even[0]:
                        continue
                    if used[1][odd[0]] >= cap or to_odd in places[1]:
                        continue
                    if steps and any(h[0] == p[0] for h, p in zip((even, odd), steps[-1][1:])):
                        continue
                    options.append((source, even, odd, to_even, to_odd))
        rnd.shuffle(options)
        options.sort(key=lambda o: o[0] + rnd.random() * 2 * len(dims))
        for source, even, odd, to_even, to_odd in options[:4]:
            now = [list(used[0]), list(used[1])]
            now[0][even[0]] += 1
            now[1][odd[0]] += 1
            found = extend(
                k + 1,
                steps + [(source, even, odd)],
                (places[0] + [to_even], places[1] + [to_odd]),
                now,
            )
            if found:
                return found
        return None

    return extend(1, [], (origin, origin), [[0] * len(dims)] * 2)


def placed(dims, order):
    hops = hops_of(dims)
    steps, places = [], ([tuple(0 for _ in dims)], [tuple(0 for _ in dims)])
    for source, even, odd in order:
        if max(even, odd) >= len(hops):
            return None
        steps.append((source, hops[even], hops[odd]))
        for core, (_, way) in enumerate(steps[-1][1:]):
            places[core].append(across(places[core][source], way))
    everywhere = set(itertools.product(*[range(n) for n in dims]))
    if any(len(p) != len(everywhere) or set(p) != everywhere for p in places):
        return None
    return steps, places


def relay(dims, tries=400):
    found, seed = placed(dims, ORDER), 0
    while not found:
        found, seed = attempt(dims, seed, tries), seed + 1
    return found


def row_of(targets, device, tok):
    lanes = targets.shape[1]
    first = device * tok
    row = first // lanes
    near = targets[pl.ds(row, 1), :]
    far = targets[pl.ds(jnp.minimum(row + 1, targets.shape[0] - 1), 1), :]
    both = jnp.broadcast_to(jnp.concatenate([near, far], axis=1), (8, 2 * lanes))
    turned = pltpu.roll(both, lax.rem(2 * lanes - (first - row * lanes), 2 * lanes), 1)
    return turned[:1, :tok]


def here():
    chip = lax.axis_index("dp") * lax.axis_size("ring") + lax.axis_index("ring")
    return chip, lax.axis_index("core"), lax.axis_size("core")


def score_kernel(count, spots, *refs):
    blocks = refs[:count]
    chip, core, cores = here()
    mine, theirs, targets, kept, stats = refs[count:]
    tok = blocks[0].shape[0]
    rows = mine.shape[0]
    groups = stats.shape[0] // 2
    left = jnp.concatenate([b[...] for b in blocks], axis=0) if count > 1 else blocks[0][...]
    stats[...] = kept[...]
    logits = []
    for table in (mine, theirs):
        logits.append(
            lax.dot_general(
                table[...], left, (((1,), (1,)), ((), ())), preferred_element_type=jnp.float32
            )
        )
    owners = [chip ^ jnp.where(core == 0, even, odd) for even, odd in spots]
    wanted = jnp.concatenate([row_of(targets, at * cores + core, tok) for at in owners], axis=1)
    maxima = functools.reduce(jnp.maximum, [jnp.max(x, axis=0, keepdims=True) for x in logits])
    totals = 0.0
    picked = 0.0
    ids = lax.broadcasted_iota(jnp.int32, logits[0].shape, 0)
    for k, x in enumerate(logits):
        totals += jnp.sum(jnp.exp(x - maxima), axis=0, keepdims=True)
        picked += jnp.sum(
            jnp.where(ids == wanted - (chip * cores + (core, cores - 1 - core)[k]) * rows, x, jnp.zeros_like(x)), axis=0, keepdims=True
        )
    level = maxima + jnp.log(totals)
    for i, at in enumerate(owners):
        stats[pl.ds(at, 1), :] = level[:, i * tok : (i + 1) * tok]
        stats[pl.ds(groups + at, 1), :] = picked[:, i * tok : (i + 1) * tok]


def score(spots, blocks, mine, theirs, targets, kept):
    count = len(blocks)
    vmem = pl.BlockSpec(memory_space=pltpu.VMEM)
    tok, width = blocks[0].shape
    rows = mine.shape[0] * 2
    return pl.pallas_call(
        functools.partial(score_kernel, count, spots),
        out_shape=jax.ShapeDtypeStruct(kept.shape, jnp.float32),
        in_specs=[vmem] * (count + 4),
        out_specs=vmem,
        cost_estimate=pl.CostEstimate(
            flops=2 * rows * width * tok * count,
            bytes_accessed=2 * width * (rows + tok * count),
            transcendentals=rows * tok * count,
        ),
        compiler_params=pltpu.CompilerParams(vmem_limit_bytes=VMEM_MIB * 2**20),
        name="score",
    )(*blocks, mine, theirs, targets, kept)


def batches_of(dims):
    total = math.prod(dims)
    early = total - len(dims)
    edges = [early * i // PIECES for i in range(PIECES + 1)] + [total]
    return [tuple(range(low, high)) for low, high in zip(edges[:-1], edges[1:])]


def tree(op, parts):
    while len(parts) > 1:
        parts = [op(*parts[i : i + 2]) if i + 1 < len(parts) else parts[i] for i in range(0, len(parts), 2)]
    return parts[0]


def joined(parts):
    half = parts[0].shape[0] // 2
    levels = [p[:half] for p in parts]
    top = tree(jnp.maximum, levels)
    total = tree(jnp.add, [jnp.exp(x - top) for x in levels])
    return top + jnp.log(total), tree(jnp.add, [p[half:] for p in parts])


def finish_kernel(mine, theirs, token_loss, mean_loss):
    token_loss[...] = mine[pl.ds(here()[0], 1), :]
    count = mine.shape[0] * mine.shape[1] * 2
    total = jnp.sum(mine[...], keepdims=True) + jnp.sum(theirs[...], keepdims=True)
    mean_loss[...] = total / count


def finish(mine, theirs):
    vmem = pl.BlockSpec(memory_space=pltpu.VMEM)
    token_loss, mean_loss = pl.pallas_call(
        finish_kernel,
        out_shape=(
            jax.ShapeDtypeStruct((1, mine.shape[1]), jnp.float32),
            jax.ShapeDtypeStruct((1, 1), jnp.float32),
        ),
        in_specs=[vmem, vmem],
        out_specs=(vmem, vmem),
        compiler_params=pltpu.CompilerParams(vmem_limit_bytes=VMEM_MIB * 2**20),
        name="finish",
    )(mine, theirs)
    return token_loss.reshape(mine.shape[1]), mean_loss.reshape(())


def local(mesh_sizes, dims, hidden, embedding, targets):
    return share(mesh_sizes, dims, hidden, embedding, targets)


def share(mesh_sizes, dims, hidden, embedding, targets):
    dp, ring, cores = mesh_sizes
    chips = dp * ring
    tok = hidden.shape[0]
    strides = [1] * len(dims)
    for k in reversed(range(len(dims) - 1)):
        strides[k] = strides[k + 1] * dims[k + 1]
    spots = [tuple(i // s % n for s, n in zip(strides, dims)) for i in range(chips)]
    index = {spot: i for i, spot in enumerate(spots)}

    def moved(array, steps, swap=False):
        pairs = []
        for i, spot in enumerate(spots):
            for c in range(cores):
                to = index[across(spot, steps[c])]
                pairs.append((i * cores + c, to * cores + (cores - 1 - c if swap else c)))
        return lax.ppermute(array, AXES, pairs)

    steps, places = relay(dims)
    still = (tuple(0 for _ in dims),) * cores
    theirs = moved(embedding, still, swap=True)

    lanes = 128
    wanted = jnp.pad(targets, (0, -targets.shape[0] % lanes)).reshape(-1, lanes)

    blocks = [hidden]
    for k, (source, even, odd) in enumerate(steps, 1):
        blocks.append(moved(blocks[source], (even[1], odd[1])))

    stats = jnp.zeros((2 * chips, tok), jnp.float32)
    for slots in batches_of(dims):
        spread = [tuple(index[p[s]] for p in places) for s in slots]
        stats = score(spread, [blocks[s] for s in slots], embedding, theirs, wanted, stats)

    long = dims.index(max(dims))
    turns = [
        [t for t in spots[1:] if not any(v for k, v in enumerate(t) if k != long)],
        [t for t in spots[1:] if not t[long]],
    ]
    for stage in reversed(turns):
        level, picked = joined([stats] + [moved(stats, (t,) * cores) for t in stage])
        stats = jnp.concatenate([level, picked], axis=0)
    losses = level - picked
    return finish(losses, moved(losses, still, swap=True))


def gathered(hidden, embedding, targets):
    tok, rows = hidden.shape[0], embedding.shape[0]
    device = lax.axis_index(AXES)
    tokens = lax.all_gather(hidden, AXES, axis=0, tiled=True)
    logits = lax.dot_general(
        tokens, embedding, (((1,), (1,)), ((), ())), preferred_element_type=jnp.float32
    )
    ids = device * rows + jnp.arange(rows, dtype=jnp.int32)
    maxima = lax.pmax(jnp.max(logits, axis=1), AXES)
    totals = jnp.sum(jnp.exp(logits - maxima[:, None]), axis=1)
    picked = jnp.sum(
        jnp.where(targets[:, None] == ids[None, :], logits, jnp.zeros_like(logits)), axis=1
    )
    totals, picked = lax.psum((totals, picked), AXES)
    losses = maxima + jnp.log(totals) - picked
    token_loss = lax.dynamic_slice_in_dim(losses, device * tok, tok)
    return token_loss, jnp.sum(losses) / losses.shape[0]


def solution(mesh):
    dp, vocab = mesh.shape["dp"], mesh.shape["vocab"]
    sizes = (dp, vocab // 2, 2)
    dims = (dp, vocab // 4, 2)
    fine = Mesh(mesh.devices.reshape(sizes), AXES)
    few = dp * vocab <= 64 and all(n & (n - 1) == 0 for n in dims)
    return jax.shard_map(
        functools.partial(local, sizes, dims) if few else gathered,
        mesh=fine,
        in_specs=(P(AXES, None), P(AXES, None), P()),
        out_specs=(P(AXES), P()),
        check_vma=False,
    )
```
